32 devices in a mesh: gx: 8 (over y, x, core), gy: 4 (over z).
Axes of the slice: x: 2, y: 2, z: 4, core: 2. Of those that a mesh axis runs over, the one named last changes fastest.
Arguments:
- objects: float32 [4, 4096, 2048], P(None, 'gx', 'gy'), may hold values from -3 to 3
- probe_wave: float32 [2, 256, 256], replicated, may hold values from -5 to 5
- prop_phase: float32 [256, 256], replicated, may hold values from -3.140625 to 3.140625
- intensity: float32 [128, 256, 256], P(('gx', 'gy')), may hold values from 0 to 1
- offsets: int32 [128, 2], P(('gx', 'gy')), may hold values from 0 to 512
- counts: int32 [32], P(('gx', 'gy')), may hold values from 1 to 4, 64 in all
Outputs:
- gradient: float32 [4, 4096, 2048], P(None, 'gx', 'gy')
The draws below stay inside these ranges and needn't reach their ends.
Inputs may be any that keep to these rules, and one draw needn't show every extreme that they name: `counts`: every device has at least one live frame; the busiest has exactly 4.
All inputs are finite; a program needn't handle non-finite values.
Results may differ from the reference program's by a relative error of at most 0.00014.
Values sent between devices are 32-bit elements; how exact they have to be, the bound alone decides.
No kernel may reach another device: no remote copies, remote signals or barrier semaphores. Data moves between devices by JAX's collectives and lax.ppermute only.
A program may use at most 128 MiB of HBM per device.

```python
import math
import jax
import jax.numpy as jnp
import numpy as np
from jax import lax

FRAME = 256
TILE = 512
CAP = 4
NX = 4096
NY = 2048
SLOTS = 128
N_GY = 4
DEVICES = 32


def plant(drawn, own_key, least, high):
    longest = drawn.shape.index(max(drawn.shape))
    spots = []
    for shift in (0, 1):
        where = [jax.random.randint(jax.random.fold_in(own_key, axis), (), 0, length) for axis, length in enumerate(drawn.shape)]
        where[longest] = (where[longest] + shift) % drawn.shape[longest]
        spots.append(tuple(where))
    return drawn.at[spots[0]].set(least).at[spots[1]].set(high)


def block_levels(key, dims, pieces, smallest, high):
    level = 1.0
    for position, parts in pieces:
        draws = jax.random.uniform(jax.random.fold_in(jax.random.fold_in(key, 6), position), (parts,), jnp.float32, smallest / len(pieces), high / len(pieces))
        level = level * jnp.repeat(jnp.exp(draws), dims[position] // parts).reshape((-1,) + (1,) * (len(dims) - 1 - position))
    return level


def split_up(number_of, total, most, skew):
    loads = [(1 << 20) // math.isqrt(standing ** skew) + 1 for standing in range(2, number_of + 1)]
    spare, holding = total - most - (number_of - 1), [1] * (number_of - 1)
    while spare > 0:
        movable = [i for i in range(number_of - 1) if holding[i] < most]
        mass, budget = sum([loads[i] for i in movable]), spare
        for i in movable:
            extra = min(most - holding[i], max(1, budget * loads[i] // mass), spare)
            holding[i] = holding[i] + extra
            spare = spare - extra
    return np.array([most] + holding)


def ragged(rng, count, total, limit, slope):
    if count == 2:
        one = jax.random.randint(rng, (), max(1, total - limit), min(limit, total - 1) + 1)
        return jnp.stack([one, total - one])
    sizes = jnp.asarray(split_up(count, total, limit, slope), jnp.int32)
    twos = (count - 1) // 2
    giver, taker = sizes[1:1 + 2 * twos:2], sizes[2:2 + 2 * twos:2]
    slack = jnp.minimum(giver - 1, limit - taker)
    shifted = jax.random.randint(jax.random.fold_in(rng, 1), (twos,), 0, 1 << 20) % (slack + 1)
    sizes = sizes.at[1:1 + 2 * twos:2].set(giver - shifted).at[2:2 + 2 * twos:2].set(taker + shifted)
    return sizes[jax.random.permutation(jax.random.fold_in(rng, 2), count)]


def normal_values(own_key, dims, width, bound, pieces=(), kind=jnp.bfloat16):
    result = width * jax.random.normal(own_key, dims, jnp.float32)
    if pieces:
        result = result * block_levels(own_key, dims, pieces, -0.22, 0.18)
    return jnp.clip(result, -bound, bound).astype(kind)


def setup_inputs(seed: int = 0) -> dict:
    seeds = jax.random.split(jax.random.key(seed), 7)
    return {
        "objects": normal_values(seeds[0], (4, NX, NY), 0.5, 3.0, ((1, 8), (2, 4)), jnp.float32),
        "probe_wave": normal_values(seeds[1], (2, FRAME, FRAME), 1.0, 5.0, (), jnp.float32),
        "prop_phase": jnp.clip(jax.random.uniform(seeds[2], (FRAME, FRAME), jnp.float32, -3.140625, 3.140625), -3.140625, 3.140625),
        "intensity": jnp.clip(1.0 * jax.random.uniform(seeds[3], (SLOTS, FRAME, FRAME), jnp.float32) ** block_levels(seeds[3], (SLOTS, FRAME, FRAME), ((0, 32),), -0.2, 0.2), 0.0, 1.0),
        "offsets": plant(jax.random.randint(seeds[4], (SLOTS, 2), 0, TILE + 1), jax.random.fold_in(seeds[4], 1), 0, TILE).astype(jnp.int32),
        "counts": ragged(seeds[5], DEVICES, DEVICES * CAP // 2, CAP, 2).astype(jnp.int32),
    }


def frame_gradient(window, measured, probe_field, propagator):
    slice_one = window[0] + 1j * window[1]
    slice_two = window[2] + 1j * window[3]
    entrance = probe_field * slice_one
    carried = jnp.fft.ifft2(propagator * jnp.fft.fft2(entrance, norm="ortho"), norm="ortho")
    exit_wave = carried * slice_two
    farfield = jnp.fft.fft2(exit_wave, norm="ortho")
    misfit = jnp.real(farfield) ** 2 + jnp.imag(farfield) ** 2 - measured
    grad_exit = jnp.fft.ifft2(misfit * farfield, norm="ortho")
    grad_two = jnp.conj(carried) * grad_exit
    grad_carried = jnp.conj(slice_two) * grad_exit
    grad_entrance = jnp.fft.ifft2(jnp.conj(propagator) * jnp.fft.fft2(grad_carried, norm="ortho"), norm="ortho")
    grad_one = jnp.conj(probe_field) * grad_entrance
    stacked = jnp.stack([jnp.real(grad_one), jnp.imag(grad_one), jnp.real(grad_two), jnp.imag(grad_two)])
    return stacked.astype(window.dtype)


def reference(objects, probe_wave, prop_phase, intensity, offsets, counts):
    margin = FRAME // 2
    padded = jnp.pad(objects, ((0, 0), (margin, margin), (margin, margin)))
    probe_field = probe_wave[0] + 1j * probe_wave[1]
    propagator = jnp.cos(prop_phase) + 1j * jnp.sin(prop_phase)
    slot_ids = jnp.arange(SLOTS, dtype=jnp.int32)
    device_ids = slot_ids // CAP
    row_starts = ((device_ids // N_GY) * TILE + offsets[:, 0]).astype(jnp.int32)
    col_starts = ((device_ids % N_GY) * TILE + offsets[:, 1]).astype(jnp.int32)
    active_slot = (slot_ids % CAP) < counts[device_ids]

    def accumulate(summed, inputs):
        measured, row_start, col_start, active = inputs
        anchor = jnp.int32(0)
        window = lax.dynamic_slice(padded, (anchor, row_start, col_start), (4, FRAME, FRAME))
        update = frame_gradient(window, measured, probe_field, propagator)
        update = jnp.where(active, update, jnp.zeros_like(update))
        current = lax.dynamic_slice(summed, (anchor, row_start, col_start), (4, FRAME, FRAME))
        return lax.dynamic_update_slice(summed, current + update, (anchor, row_start, col_start)), None

    summed, unused = lax.scan(accumulate, jnp.zeros_like(padded), (intensity, row_starts, col_starts, active_slot))
    return summed[:, margin:margin + NX, margin:margin + NY]
```

```python
import math

import jax
import jax.numpy as jnp
import numpy as np
from jax import lax
from jax.experimental import pallas as pl
from jax.experimental.pallas import tpu as pltpu
from jax.sharding import PartitionSpec as P


ROWS = 32


def half_tables(frame):
    half = frame // 2
    n = np.arange(half)
    angle = 2.0 * np.pi * ((n[:, None] * n[None, :]) % half) / half
    scale = 1.0 / math.sqrt(frame)
    c, s = np.cos(angle) * scale, np.sin(angle) * scale
    right = np.block([[c, -s], [s, c]])
    turn = 2.0 * np.pi * n / frame
    return right, np.cos(turn), np.sin(turn)


def split_const(m):
    hi = m.astype(np.float32).astype(jnp.bfloat16)
    lo = (m - hi.astype(np.float64)).astype(np.float32).astype(jnp.bfloat16)
    return hi, lo


def put(hi_ref, lo_ref, rows, cols, value):
    hi = value.astype(jnp.bfloat16)
    hi_ref[rows, cols] = hi
    lo_ref[rows, cols] = (value - hi.astype(jnp.float32)).astype(jnp.bfloat16)


def mm(left, right):
    return jnp.dot(left, right, preferred_element_type=jnp.float32)


def cmul(ar, ai, br, bi):
    return ar * br - ai * bi, ar * bi + ai * br


def cmul_conj(ar, ai, br, bi):
    return ar * br + ai * bi, ar * bi - ai * br


def frame_kernel(
    scal, tile, left, right, over, lcor, rcor, ext_e, inten, probe, prop, mats, twl, twc,
    g_tile, g_left, g_right, g_over, g_ext, g_ol, g_or, g_el, g_er,
    obj, acc, win, car, fld, lh, ll, rh, rl, dd, sems,
):
    frame = probe.shape[1]
    half = frame // 2
    size = tile.shape[1]
    ntile = size // half
    even = scal[1] == 0
    e_row = jnp.where(even, half + size, 0)
    o_row = jnp.where(even, 0, half + size)
    e_row = pl.multiple_of(e_row, half)
    o_row = pl.multiple_of(o_row, half)
    mid = pl.ds(half, size)

    def blocks(array, width):
        return [array.at[:, :, pl.ds(half * j, half)] for j in range(width)]

    def moves(big, t, l, r, o, ol, orr, e, el, er):
        pairs = [
            (l, big.at[:, 0, mid, :]),
            (r, big.at[:, ntile + 1, mid, :]),
            (ol, big.at[:, 0, pl.ds(o_row, half), :]),
            (orr, big.at[:, ntile + 1, pl.ds(o_row, half), :]),
            (el, big.at[:, 0, pl.ds(e_row, half), :]),
            (er, big.at[:, ntile + 1, pl.ds(e_row, half), :]),
        ]
        for j in range(ntile):
            pairs.append((o[j], big.at[:, j + 1, pl.ds(o_row, half), :]))
            pairs.append((e[j], big.at[:, j + 1, pl.ds(e_row, half), :]))
            pairs.append((t[j], big.at[:, j + 1, mid, :]))
        return pairs

    strip = blocks(ext_e, ntile + 2)
    loads = [
        pltpu.make_async_copy(src, dst, sems.at[i])
        for i, (src, dst) in enumerate(
            moves(
                obj, blocks(tile, ntile), left, right, blocks(over, ntile), lcor, rcor,
                strip[1:-1], strip[0], strip[-1],
            )
        )
    ]
    for copy in loads:
        copy.start()

    def clear(i, carry):
        acc[i // (ntile + 2), i % (ntile + 2)] = jnp.zeros(acc.shape[2:], jnp.float32)
        return carry

    lax.fori_loop(0, acc.shape[0] * (ntile + 2), clear, 0)
    for copy in loads:
        copy.wait()

    lane = lax.broadcasted_iota(jnp.int32, (ROWS, half), 1)
    low, high = slice(0, half), slice(half, frame)

    def right_forward(source):
        for rb in range(0, frame, ROWS):
            rows = slice(rb, rb + ROWS)
            xr, xi = source(rows)
            ar, br, ai, bi = xr[:, :half], xr[:, half:], xi[:, :half], xi[:, half:]
            put(lh, ll, rows, low, ar + br)
            put(lh, ll, rows, high, ai + bi)
            dr, di = ar - br, ai - bi
            c, s = twl[0:1, :], twl[1:2, :]
            vrows = slice(frame + rb, frame + rb + ROWS)
            put(lh, ll, vrows, low, dr * c + di * s)
            put(lh, ll, vrows, high, di * c - dr * s)
        dd[...] = mm(lh[...], mats[0]) + mm(ll[...], mats[0]) + mm(lh[...], mats[1])

    def left_forward():
        for q in range(2):
            for rb in range(0, half, ROWS):
                rows = slice(rb, rb + ROWS)
                t = pl.ds(q * frame + rb, ROWS)
                b = pl.ds(q * frame + half + rb, ROWS)
                ar, ai, br, bi = dd[t, low], dd[t, high], dd[b, low], dd[b, high]
                irows = slice(half + rb, half + rb + ROWS)
                ucols = slice(q * half, (q + 1) * half)
                vcols = slice(frame + q * half, frame + (q + 1) * half)
                put(rh, rl, rows, ucols, ar + br)
                put(rh, rl, irows, ucols, ai + bi)
                dr, di = ar - br, ai - bi
                c, s = twc[0, rows, :], twc[1, rows, :]
                put(rh, rl, rows, vcols, dr * c + di * s)
                put(rh, rl, irows, vcols, di * c - dr * s)
        return mm(mats[2], rh[...]) + mm(mats[2], rl[...]) + mm(mats[3], rh[...])

    def forward(source):
        right_forward(source)
        fld[...] = left_forward()

    def inverse(source, sink):
        for rb in range(0, half, ROWS):
            rows = slice(rb, rb + ROWS)
            xr, xi = source(rows)
            put(rh, rl, rows, slice(None), xr)
            put(rh, rl, slice(half + rb, half + rb + ROWS), slice(None), xi)
        fld[...] = mm(mats[0], rh[...]) + mm(mats[0], rl[...]) + mm(mats[1], rh[...])
        for q in range(2):
            for rb in range(0, half, ROWS):
                rows = slice(rb, rb + ROWS)
                irows = slice(half + rb, half + rb + ROWS)
                ecols = slice(q * half, (q + 1) * half)
                ocols = slice(frame + q * half, frame + (q + 1) * half)
                er, ei, wr, wi = fld[rows, ecols], fld[irows, ecols], fld[rows, ocols], fld[irows, ocols]
                c, s = twc[0, rows, :], twc[1, rows, :]
                tr, ti = wr * c - wi * s, wi * c + wr * s
                top = slice(q * frame + rb, q * frame + rb + ROWS)
                bot = slice(q * frame + half + rb, q * frame + half + rb + ROWS)
                put(lh, ll, top, low, er + tr)
                put(lh, ll, top, high, ei + ti)
                put(lh, ll, bot, low, er - tr)
                put(lh, ll, bot, high, ei - ti)
        dd[...] = mm(lh[...], mats[2]) + mm(ll[...], mats[2]) + mm(lh[...], mats[3])
        for rb in range(0, frame, ROWS):
            rows = slice(rb, rb + ROWS)
            orows = slice(frame + rb, frame + rb + ROWS)
            er, ei, wr, wi = dd[rows, low], dd[rows, high], dd[orows, low], dd[orows, high]
            c, s = twl[0:1, :], twl[1:2, :]
            tr, ti = wr * c - wi * s, wi * c + wr * s
            sink(rows, er + tr, ei + ti, er - tr, ei - ti)

    def step(f, carry):
        r = scal[2 + 2 * f]
        c = scal[3 + 2 * f]
        j = jnp.minimum(c // half, ntile - 1)
        cs = c - j * half
        back = lax.rem(half - cs, half)
        fore = lax.rem(cs, half)
        keep = lane + cs < half
        spill = lane >= cs

        for k in range(4):
            for rb in range(0, frame, ROWS):
                parts = [
                    pltpu.roll(obj[k, j + t, pl.ds(r + rb, ROWS), :], back, 1) for t in range(3)
                ]
                win[k, rb:rb + ROWS, low] = jnp.where(keep, parts[0], parts[1])
                win[k, rb:rb + ROWS, high] = jnp.where(keep, parts[1], parts[2])

        def place(k, rows, first, second):
            a, b = pltpu.roll(first, fore, 1), pltpu.roll(second, fore, 1)
            at = pl.ds(r + rows.start, ROWS)
            zero = jnp.zeros_like(a)
            acc[k, j, at, :] += jnp.where(spill, a, zero)
            acc[k, j + 1, at, :] += jnp.where(spill, b, a)
            acc[k, j + 2, at, :] += jnp.where(spill, zero, b)

        def enter(rows):
            return cmul(probe[0, rows, :], probe[1, rows, :], win[0, rows, :], win[1, rows, :])

        def lower(rows):
            return slice(half + rows.start, half + rows.stop)

        def propagate(rows):
            return cmul(prop[0, rows, :], prop[1, rows, :], fld[rows, :], fld[lower(rows), :])

        def propagate_back(rows):
            return cmul_conj(prop[0, rows, :], prop[1, rows, :], fld[rows, :], fld[lower(rows), :])

        def carried(rows, ar, ai, br, bi):
            car[0, rows, low] = ar
            car[1, rows, low] = ai
            car[0, rows, high] = br
            car[1, rows, high] = bi

        def exit_wave(rows):
            return cmul(car[0, rows, :], car[1, rows, :], win[2, rows, :], win[3, rows, :])

        def misfit(rows):
            fr, fi = fld[rows, :], fld[lower(rows), :]
            m = fr * fr + fi * fi - inten[f, rows, :]
            return m * fr, m * fi

        def grad_exit(rows, ar, ai, br, bi):
            lr, li = cmul_conj(car[0, rows, low], car[1, rows, low], ar, ai)
            hr, hi = cmul_conj(car[0, rows, high], car[1, rows, high], br, bi)
            place(2, rows, lr, hr)
            place(3, rows, li, hi)
            for cols, (gr, gi) in ((low, (ar, ai)), (high, (br, bi))):
                xr, xi = cmul_conj(win[2, rows, cols], win[3, rows, cols], gr, gi)
                win[0, rows, cols] = xr
                win[1, rows, cols] = xi

        def grad_enter(rows, ar, ai, br, bi):
            lr, li = cmul_conj(probe[0, rows, low], probe[1, rows, low], ar, ai)
            hr, hi = cmul_conj(probe[0, rows, high], probe[1, rows, high], br, bi)
            place(0, rows, lr, hr)
            place(1, rows, li, hi)

        forward(enter)
        inverse(propagate, carried)
        forward(exit_wave)
        inverse(misfit, grad_exit)
        forward(lambda rows: (win[0, rows, :], win[1, rows, :]))
        inverse(propagate_back, grad_enter)
        return carry

    lax.fori_loop(0, scal[0], step, 0)

    stores = [
        pltpu.make_async_copy(src, dst, sems.at[i])
        for i, (dst, src) in enumerate(
            moves(
                acc, blocks(g_tile, ntile), g_left, g_right, blocks(g_over, ntile), g_ol, g_or,
                blocks(g_ext, ntile), g_el, g_er,
            )
        )
    ]
    for copy in stores:
        copy.start()
    for copy in stores:
        copy.wait()


def run_frames(scal, pieces, inten, probe, prop, frame):
    right, tc, ts = half_tables(frame)
    half = frame // 2
    rhi, rlo = split_const(right)
    mats = np.stack([rhi, rlo, np.ascontiguousarray(rhi.T), np.ascontiguousarray(rlo.T)])
    twl = np.zeros((8, half), np.float32)
    twl[0], twl[1] = tc, ts
    twc = np.stack([np.repeat(tc[:, None], half, 1), np.repeat(ts[:, None], half, 1)]).astype(np.float32)
    channels, size, _ = pieces[0].shape
    ntile = size // half
    hbm = pl.BlockSpec(memory_space=pl.ANY)
    vmem = pl.BlockSpec(memory_space=pltpu.VMEM)
    big = (channels, ntile + 2, size + frame, half)
    tile, left, right, over, lcor, rcor, _ = pieces
    outs = [
        jax.ShapeDtypeStruct(p.shape, jnp.float32)
        for p in (tile, left, right, over, over, lcor, rcor, lcor, rcor)
    ]
    copies = 3 * ntile + 6
    return pl.pallas_call(
        frame_kernel,
        out_shape=outs,
        in_specs=[pl.BlockSpec(memory_space=pltpu.SMEM)] + [hbm] * len(pieces) + [vmem] * 6,
        out_specs=[hbm] * len(outs),
        scratch_shapes=[
            pltpu.VMEM(big, jnp.float32),
            pltpu.VMEM(big, jnp.float32),
            pltpu.VMEM((4, frame, frame), jnp.float32),
            pltpu.VMEM((2, frame, frame), jnp.float32),
            pltpu.VMEM((frame, 2 * frame), jnp.float32),
            pltpu.VMEM((2 * frame, frame), jnp.bfloat16),
            pltpu.VMEM((2 * frame, frame), jnp.bfloat16),
            pltpu.VMEM((frame, 2 * frame), jnp.bfloat16),
            pltpu.VMEM((frame, 2 * frame), jnp.bfloat16),
            pltpu.VMEM((2 * frame, frame), jnp.float32),
            pltpu.SemaphoreType.DMA((copies,)),
        ],
        compiler_params=pltpu.CompilerParams(vmem_limit_bytes=40 * 1024 * 1024),
        cost_estimate=pl.CostEstimate(flops=40_000_000_000, bytes_accessed=30_000_000, transcendentals=0),
        name="frames",
    )(scal, *pieces, inten, probe, prop, mats, twl, twc)


def parity_kernel(inten, prop, pick, inten_out, prop_out, mid):
    half = pick.shape[0] // 2

    def sort(src, dst, index):
        x = src[index]
        top = x.astype(jnp.bfloat16)
        rest = x - top.astype(jnp.float32)
        middle = rest.astype(jnp.bfloat16)
        last = (rest - middle.astype(jnp.float32)).astype(jnp.bfloat16)
        out = mm(top, pick[...]) + mm(middle, pick[...]) + mm(last, pick[...])
        mid[2 * index] = out[:, :half]
        mid[2 * index + 1] = out[:, half:]
        for q in range(2):
            for p in range(2):
                cols = slice((2 * q + p) * half, (2 * q + p + 1) * half)
                dst[index, :, cols] = mid[2 * index + p, pl.ds(q, half, stride=2), :]

    for i in range(inten.shape[0]):
        sort(inten, inten_out, i)
    for i in range(prop.shape[0]):
        sort(prop, prop_out, i)


def by_parity(inten, prop):
    frame = inten.shape[-1]
    half = frame // 2
    pick = np.zeros((frame, frame), np.float32)
    n = np.arange(half)
    pick[2 * n, n] = 1.0
    pick[2 * n + 1, half + n] = 1.0
    vmem = pl.BlockSpec(memory_space=pltpu.VMEM)
    return pl.pallas_call(
        parity_kernel,
        out_shape=[
            jax.ShapeDtypeStruct((x.shape[0], half, 2 * frame), jnp.float32) for x in (inten, prop)
        ],
        in_specs=[vmem] * 3,
        out_specs=[vmem] * 2,
        scratch_shapes=[pltpu.VMEM((2 * inten.shape[0], frame, half), jnp.float32)],
        cost_estimate=pl.CostEstimate(flops=4_000_000_000, bytes_accessed=3_000_000, transcendentals=0),
        name="parity",
    )(inten, prop, pick.astype(jnp.bfloat16))


def pair_route(count, first):
    route = []
    for i in range(first, count - 1, 2):
        route += [(i, i + 1), (i + 1, i)]
    return route


def shards(objects, probe_wave, prop_phase, intensity, offsets, counts):
    frame = intensity.shape[1]
    margin = frame // 2
    size_r, size_c = objects.shape[1:]
    nx, ny = lax.axis_size("gx"), lax.axis_size("gy")
    parity = lax.axis_index("gx") % 2
    to_left = [(i, i - 1) for i in range(1, ny)]
    to_right = [(i, i + 1) for i in range(ny - 1)]
    e_route, o_route = pair_route(nx, 0), pair_route(nx, 1)
    e_start = jnp.where(parity == 0, size_r - margin, 0)
    o_start = jnp.where(parity == 0, 0, size_r - margin)

    def band(x, start):
        return lax.dynamic_slice_in_dim(x, start, margin, 1)

    def corner(x_route, y_route):
        return [(a * ny + c, b * ny + d) for a, b in x_route for c, d in y_route]

    def add_at(x, row, col, update):
        at = (0, row, col)
        old = lax.dynamic_slice(x, at, update.shape)
        return lax.dynamic_update_slice(x, old + update, at)

    over = lax.ppermute(band(objects, o_start), "gx", o_route)
    right = lax.ppermute(objects[:, :, :margin], "gy", to_left)
    left = lax.ppermute(objects[:, :, -margin:], "gy", to_right)
    first, last = over[:, :, :margin], over[:, :, -margin:]
    rcor = lax.ppermute(first, "gy", to_left)
    lcor = lax.ppermute(last, "gy", to_right)
    strip = jnp.concatenate([band(left, e_start), band(objects, e_start), band(right, e_start)], axis=2)
    ext = lax.ppermute(strip, "gx", e_route)

    waves = jnp.stack([jnp.cos(prop_phase), jnp.sin(prop_phase)])
    inten, waves = by_parity(intensity, waves)
    scal = jnp.concatenate([counts, parity[None].astype(jnp.int32), offsets.reshape(-1)])
    pieces = [objects, left, right, over, lcor, rcor, ext]
    tile, left, right, over, ext, ol, orr, el, er = run_frames(
        scal, pieces, inten, probe_wave, waves, frame
    )

    both = ("gx", "gy")
    from_right = lax.ppermute(left, "gy", to_left)
    from_left = lax.ppermute(right, "gy", to_right)
    over = lax.ppermute(over, "gx", o_route)
    ext = lax.ppermute(ext, "gx", e_route)
    ol = lax.ppermute(ol, both, corner(o_route, to_left))
    orr = lax.ppermute(orr, both, corner(o_route, to_right))
    el = lax.ppermute(el, both, corner(e_route, to_left))
    er = lax.ppermute(er, both, corner(e_route, to_right))
    far = size_c - margin
    tile = add_at(tile, e_start, 0, ext)
    tile = add_at(tile, o_start, 0, over)
    tile = add_at(tile, 0, far, from_right)
    tile = add_at(tile, 0, 0, from_left)
    tile = add_at(tile, o_start, far, ol)
    tile = add_at(tile, o_start, 0, orr)
    tile = add_at(tile, e_start, far, el)
    return add_at(tile, e_start, 0, er)


def solution(mesh):
    return jax.shard_map(
        shards,
        mesh=mesh,
        in_specs=(
            P(None, "gx", "gy"),
            P(),
            P(),
            P(("gx", "gy"), None, None),
            P(("gx", "gy"), None),
            P(("gx", "gy")),
        ),
        out_specs=P(None, "gx", "gy"),
        check_vma=False,
    )
```

```python
import math

import jax
import jax.numpy as jnp
import numpy as np
from jax import lax
from jax.experimental import pallas as pl
from jax.experimental.pallas import tpu as pltpu
from jax.sharding import PartitionSpec as P


ROWS = 32


def half_tables(frame):
    half = frame // 2
    n = np.arange(half)
    angle = 2.0 * np.pi * ((n[:, None] * n[None, :]) % half) / half
    scale = 1.0 / math.sqrt(frame)
    c, s = np.cos(angle) * scale, np.sin(angle) * scale
    right = np.block([[c, -s], [s, c]])
    turn = 2.0 * np.pi * n / frame
    return right, np.cos(turn), np.sin(turn)


def split_const(m):
    hi = m.astype(np.float32).astype(jnp.bfloat16)
    lo = (m - hi.astype(np.float64)).astype(np.float32).astype(jnp.bfloat16)
    return hi, lo


def mm(left, right):
    return jnp.dot(left, right, preferred_element_type=jnp.float32)


def cmul(ar, ai, br, bi):
    return ar * br - ai * bi, ar * bi + ai * br


def cmul_conj(ar, ai, br, bi):
    return ar * br + ai * bi, ar * bi - ai * br


def frame_kernel(
    scal, tile, left, right, over, oedge, ext_e, lcor, rcor, ecor, inten_in, probe_in, prop_in, mats_in, twl_in, twc_in,
    g_tile, g_lmain, g_rmain, g_ledge, g_redge, g_over, g_oedge, g_ext, g_ol, g_or,
    obj, acc, win, car, fld, lh, ll, rh, rl, dd, inten, probe, prop, mats, twl, twc, sems,
):
    frame = probe.shape[1]
    cap = inten.shape[0]
    half = frame // 2
    size = tile.shape[1]
    ntile = size // half
    even = scal[1] == 0
    e_row = jnp.where(even, half + size, 0)
    o_row = jnp.where(even, 0, half + size)
    e_row = pl.multiple_of(e_row, half)
    o_row = pl.multiple_of(o_row, half)
    mid = pl.ds(half, size)

    def blocks(array, width):
        return [array.at[:, :, pl.ds(half * j, half)] for j in range(width)]

    m_row = pl.multiple_of(jnp.where(even, half, frame), half)
    edge_row = pl.multiple_of(jnp.where(even, size, half), half)
    o_rows, e_rows = pl.ds(o_row, half), pl.ds(e_row, half)
    m_rows, edge_rows = pl.ds(m_row, size - half), pl.ds(edge_row, half)
    last = ntile + 1

    def moves(big, t, o, ol, orr, e):
        pairs = [(ol, big.at[:, 0, o_rows, :]), (orr, big.at[:, last, o_rows, :])]
        for j in range(ntile):
            pairs.append((o[j], big.at[:, j + 1, o_rows, :]))
            pairs.append((t[j], big.at[:, j + 1, mid, :]))
        for j in range(ntile + 2):
            pairs.append((e[j], big.at[:, j, e_rows, :]))
        return pairs

    def o_blocks(middle, ends):
        return [ends.at[0]] + blocks(middle, ntile - 2) + [ends.at[1]]

    routes = moves(
        obj, blocks(tile, ntile), o_blocks(over, oedge), lcor, rcor,
        [ecor.at[0]] + blocks(ext_e, ntile) + [ecor.at[1]],
    ) + [
        (left, obj.at[:, 0, mid, :]), (right, obj.at[:, last, mid, :]),
        (inten_in, inten), (probe_in, probe), (prop_in, prop), (mats_in, mats), (twl_in, twl), (twc_in, twc)
    ]
    loads = [pltpu.make_async_copy(src, dst, sems.at[i]) for i, (src, dst) in enumerate(routes)]
    for copy in loads:
        copy.start()

    def clear(i, carry):
        acc[i // (ntile + 2), i % (ntile + 2)] = jnp.zeros(acc.shape[2:], jnp.float32)
        return carry

    lax.fori_loop(0, acc.shape[0] * (ntile + 2), clear, 0)
    for copy in loads:
        copy.wait()

    lane = lax.broadcasted_iota(jnp.int32, (ROWS, half), 1)
    low, high = slice(0, half), slice(half, frame)

    def put(hi_ref, lo_ref, u, rows, cols, value):
        hi = value.astype(jnp.bfloat16)
        hi_ref[u, rows, cols] = hi
        lo_ref[u, rows, cols] = (value - hi.astype(jnp.float32)).astype(jnp.bfloat16)

    def right_product(u, m):
        dd[u] = mm(lh[u], mats[m]) + mm(ll[u], mats[m]) + mm(lh[u], mats[m + 1])

    def left_product(u, m):
        fld[u] = mm(mats[m], rh[u]) + mm(mats[m], rl[u]) + mm(mats[m + 1], rh[u])

    def right_forward(u, source):
        for rb in range(0, frame, ROWS):
            rows = slice(rb, rb + ROWS)
            xr, xi = source(u, rows)
            ar, br, ai, bi = xr[:, :half], xr[:, half:], xi[:, :half], xi[:, half:]
            put(lh, ll, u, rows, low, ar + br)
            put(lh, ll, u, rows, high, ai + bi)
            dr, di = ar - br, ai - bi
            c, s = twl[0:1, :], twl[1:2, :]
            vrows = slice(frame + rb, frame + rb + ROWS)
            put(lh, ll, u, vrows, low, dr * c + di * s)
            put(lh, ll, u, vrows, high, di * c - dr * s)
        right_product(u, 0)

    def left_forward(u):
        for q in range(2):
            for rb in range(0, half, ROWS):
                rows = slice(rb, rb + ROWS)
                t = slice(q * frame + rb, q * frame + rb + ROWS)
                b = slice(q * frame + half + rb, q * frame + half + rb + ROWS)
                ar, ai, br, bi = dd[u, t, low], dd[u, t, high], dd[u, b, low], dd[u, b, high]
                irows = slice(half + rb, half + rb + ROWS)
                ucols = slice(q * half, (q + 1) * half)
                vcols = slice(frame + q * half, frame + (q + 1) * half)
                put(rh, rl, u, rows, ucols, ar + br)
                put(rh, rl, u, irows, ucols, ai + bi)
                dr, di = ar - br, ai - bi
                c, s = twc[0, rows, :], twc[1, rows, :]
                put(rh, rl, u, rows, vcols, dr * c + di * s)
                put(rh, rl, u, irows, vcols, di * c - dr * s)
        left_product(u, 2)

    def left_inverse(u, source):
        for rb in range(0, half, ROWS):
            rows = slice(rb, rb + ROWS)
            xr, xi = source(u, rows)
            put(rh, rl, u, rows, slice(None), xr)
            put(rh, rl, u, slice(half + rb, half + rb + ROWS), slice(None), xi)
        left_product(u, 0)

    def right_inverse(u):
        for q in range(2):
            for rb in range(0, half, ROWS):
                rows = slice(rb, rb + ROWS)
                irows = slice(half + rb, half + rb + ROWS)
                ecols = slice(q * half, (q + 1) * half)
                ocols = slice(frame + q * half, frame + (q + 1) * half)
                er, ei = fld[u, rows, ecols], fld[u, irows, ecols]
                wr, wi = fld[u, rows, ocols], fld[u, irows, ocols]
                c, s = twc[0, rows, :], twc[1, rows, :]
                tr, ti = wr * c - wi * s, wi * c + wr * s
                top = slice(q * frame + rb, q * frame + rb + ROWS)
                bot = slice(q * frame + half + rb, q * frame + half + rb + ROWS)
                put(lh, ll, u, top, low, er + tr)
                put(lh, ll, u, top, high, ei + ti)
                put(lh, ll, u, bot, low, er - tr)
                put(lh, ll, u, bot, high, ei - ti)
        right_product(u, 2)

    def finish(u, sink):
        for rb in range(0, frame, ROWS):
            rows = slice(rb, rb + ROWS)
            orows = slice(frame + rb, frame + rb + ROWS)
            er, ei, wr, wi = dd[u, rows, low], dd[u, rows, high], dd[u, orows, low], dd[u, orows, high]
            c, s = twl[0:1, :], twl[1:2, :]
            tr, ti = wr * c - wi * s, wi * c + wr * s
            sink(u, rows, er + tr, ei + ti, er - tr, ei - ti)

    def step(i, carry):
        first = 2 * i
        slots = (first, jnp.minimum(first + 1, cap - 1))
        live = (None, first + 1 < scal[0])
        spots = []
        for slot in slots:
            r, c = scal[2 + 2 * slot], scal[3 + 2 * slot]
            j = jnp.minimum(c // half, ntile - 1)
            cs = c - j * half
            spots.append((r, j, cs, lax.rem(half - cs, half), lax.rem(cs, half)))

        def load(u, k):
            r, j, cs, back, _ = spots[u]
            keep = lane + cs < half
            for rb in range(0, frame, ROWS):
                parts = [
                    pltpu.roll(obj[k, j + t, pl.ds(r + rb, ROWS), :], back, 1) for t in range(3)
                ]
                win[u, k, rb:rb + ROWS, low] = jnp.where(keep, parts[0], parts[1])
                win[u, k, rb:rb + ROWS, high] = jnp.where(keep, parts[1], parts[2])

        def place(u, k, rows, first, second):
            r, j, cs, _, fore = spots[u]
            zero = jnp.zeros_like(first)
            if live[u] is not None:
                first = jnp.where(live[u], first, zero)
                second = jnp.where(live[u], second, zero)
            spill = lane >= cs
            a, b = pltpu.roll(first, fore, 1), pltpu.roll(second, fore, 1)
            at = pl.ds(r + rows.start, ROWS)
            acc[k, j, at, :] += jnp.where(spill, a, zero)
            acc[k, j + 1, at, :] += jnp.where(spill, b, a)
            acc[k, j + 2, at, :] += jnp.where(spill, zero, b)

        def lower(rows):
            return slice(half + rows.start, half + rows.stop)

        def enter(u, rows):
            return cmul(probe[0, rows, :], probe[1, rows, :], win[u, 0, rows, :], win[u, 1, rows, :])

        def propagate(u, rows):
            return cmul(prop[0, rows, :], prop[1, rows, :], fld[u, rows, :], fld[u, lower(rows), :])

        def propagate_back(u, rows):
            return cmul_conj(prop[0, rows, :], prop[1, rows, :], fld[u, rows, :], fld[u, lower(rows), :])

        def carried(u, rows, ar, ai, br, bi):
            car[u, 0, rows, low] = ar
            car[u, 1, rows, low] = ai
            car[u, 0, rows, high] = br
            car[u, 1, rows, high] = bi

        def exit_wave(u, rows):
            return cmul(car[u, 0, rows, :], car[u, 1, rows, :], win[u, 2, rows, :], win[u, 3, rows, :])

        def misfit(u, rows):
            fr, fi = fld[u, rows, :], fld[u, lower(rows), :]
            m = fr * fr + fi * fi - inten[slots[u], rows, :]
            return m * fr, m * fi

        def grad_exit(u, rows, ar, ai, br, bi):
            lr, li = cmul_conj(car[u, 0, rows, low], car[u, 1, rows, low], ar, ai)
            hr, hi = cmul_conj(car[u, 0, rows, high], car[u, 1, rows, high], br, bi)
            place(u, 2, rows, lr, hr)
            place(u, 3, rows, li, hi)
            for cols, (gr, gi) in ((low, (ar, ai)), (high, (br, bi))):
                xr, xi = cmul_conj(win[u, 2, rows, cols], win[u, 3, rows, cols], gr, gi)
                win[u, 0, rows, cols] = xr
                win[u, 1, rows, cols] = xi

        def inner(u, rows):
            return win[u, 0, rows, :], win[u, 1, rows, :]

        def grad_enter(u, rows, ar, ai, br, bi):
            lr, li = cmul_conj(probe[0, rows, low], probe[1, rows, low], ar, ai)
            hr, hi = cmul_conj(probe[0, rows, high], probe[1, rows, high], br, bi)
            place(u, 0, rows, lr, hr)
            place(u, 1, rows, li, hi)

        both = (0, 1)
        phases = [
            lambda u: [load(u, 0), load(u, 1), right_forward(u, enter)],
            left_forward,
            lambda u: left_inverse(u, propagate),
            right_inverse,
            lambda u: [finish(u, carried), load(u, 2), load(u, 3), right_forward(u, exit_wave)],
            left_forward,
            lambda u: left_inverse(u, misfit),
            right_inverse,
            lambda u: [finish(u, grad_exit), right_forward(u, inner)],
            left_forward,
            lambda u: left_inverse(u, propagate_back),
            right_inverse,
            lambda u: finish(u, grad_enter),
        ]
        for phase in phases:
            for u in both:
                phase(u)
        return carry

    lax.fori_loop(0, (scal[0] + 1) // 2, step, 0)

    targets = moves(
        acc, blocks(g_tile, ntile), o_blocks(g_over, g_oedge), g_ol, g_or, blocks(g_ext, ntile + 2)
    ) + [
        (g_lmain, acc.at[:, 0, m_rows, :]), (g_rmain, acc.at[:, last, m_rows, :]),
        (g_ledge, acc.at[:, 0, edge_rows, :]), (g_redge, acc.at[:, last, edge_rows, :]),
    ]
    stores = [pltpu.make_async_copy(src, dst, sems.at[i]) for i, (dst, src) in enumerate(targets)]
    for copy in stores:
        copy.start()
    for copy in stores:
        copy.wait()


def run_frames(scal, pieces, inten, probe, prop, frame):
    right, tc, ts = half_tables(frame)
    half = frame // 2
    rhi, rlo = split_const(right)
    mats = np.stack([rhi, rlo, np.ascontiguousarray(rhi.T), np.ascontiguousarray(rlo.T)])
    twl = np.zeros((8, half), np.float32)
    twl[0], twl[1] = tc, ts
    twc = np.stack([np.repeat(tc[:, None], half, 1), np.repeat(ts[:, None], half, 1)]).astype(np.float32)
    channels, size, _ = pieces[0].shape
    ntile = size // half
    hbm = pl.BlockSpec(memory_space=pl.ANY)
    vmem = pl.BlockSpec(memory_space=pltpu.VMEM)
    big = (channels, ntile + 2, size + frame, half)
    tile, _, _, over, oedge, _, cor = pieces[:7]
    main = (channels, size - half, half)
    strip = (channels, half, size + frame)
    outs = [
        jax.ShapeDtypeStruct(shape, jnp.float32)
        for shape in (
            tile.shape, main, main, cor.shape, cor.shape, over.shape, oedge.shape, strip, cor.shape, cor.shape
        )
    ]
    operands = (inten, probe, prop, mats, twl, twc)
    copies = 3 * ntile + 8 + len(operands)
    return pl.pallas_call(
        frame_kernel,
        out_shape=outs,
        in_specs=[pl.BlockSpec(memory_space=pltpu.SMEM)] + [hbm] * len(pieces) + [pl.BlockSpec(memory_space=pltpu.HBM)] * len(operands),
        out_specs=[hbm] * len(outs),
        scratch_shapes=[
            pltpu.VMEM(big, jnp.float32),
            pltpu.VMEM(big, jnp.float32),
            pltpu.VMEM((2, 4, frame, frame), jnp.float32),
            pltpu.VMEM((2, 2, frame, frame), jnp.float32),
            pltpu.VMEM((2, frame, 2 * frame), jnp.float32),
            pltpu.VMEM((2, 2 * frame, frame), jnp.bfloat16),
            pltpu.VMEM((2, 2 * frame, frame), jnp.bfloat16),
            pltpu.VMEM((2, frame, 2 * frame), jnp.bfloat16),
            pltpu.VMEM((2, frame, 2 * frame), jnp.bfloat16),
            pltpu.VMEM((2, 2 * frame, frame), jnp.float32),
        ]
        + [pltpu.VMEM(x.shape, x.dtype) for x in operands]
        + [pltpu.SemaphoreType.DMA((copies,))],
        compiler_params=pltpu.CompilerParams(vmem_limit_bytes=36 * 1024 * 1024),
        cost_estimate=pl.CostEstimate(flops=40_000_000_000, bytes_accessed=30_000_000, transcendentals=0),
        name="frames",
    )(scal, *pieces, *operands)


def merge_kernel(scal, tile, right, left, redge, ledge, over, oedge, ext, out, stage, sems):
    channels, size, _ = stage.shape
    w = right.shape[2]
    even = scal[1] == 0
    far = size - w
    e_row = pl.multiple_of(jnp.where(even, far, 0), w)
    o_row = pl.multiple_of(jnp.where(even, 0, far), w)
    m_row = pl.multiple_of(jnp.where(even, 0, w), w)
    lo, mid, hi = slice(0, w), slice(w, far), slice(far, size)
    e_rows, o_rows, m_rows = pl.ds(e_row, w), pl.ds(o_row, w), pl.ds(m_row, far)
    copies = []
    for k in range(channels):
        stage[k] = tile[k]
        stage[k, m_rows, hi] += right[k]
        stage[k, m_rows, lo] += left[k]
        stage[k, o_rows, mid] += over[k]
        stage[k, o_rows, lo] += oedge[0, k]
        stage[k, o_rows, hi] += oedge[1, k]
        stage[k, e_rows, :] += ext[k, :, w:-w]
        stage[k, e_rows, hi] += redge[k]
        stage[k, e_rows, lo] += ledge[k]
        copy = pltpu.make_async_copy(stage.at[k], out.at[k], sems.at[k])
        copy.start()
        copies.append(copy)
    for copy in copies:
        copy.wait()


def merge(scal, tile, *parts):
    vmem = pl.BlockSpec(memory_space=pltpu.VMEM)
    return pl.pallas_call(
        merge_kernel,
        out_shape=jax.ShapeDtypeStruct(tile.shape, jnp.float32),
        in_specs=[pl.BlockSpec(memory_space=pltpu.SMEM)] + [vmem] * (1 + len(parts)),
        out_specs=pl.BlockSpec(memory_space=pl.ANY),
        scratch_shapes=[
            pltpu.VMEM(tile.shape, jnp.float32),
            pltpu.SemaphoreType.DMA((tile.shape[0],)),
        ],
        compiler_params=pltpu.CompilerParams(vmem_limit_bytes=20 * 1024 * 1024),
        cost_estimate=pl.CostEstimate(flops=10_000_000, bytes_accessed=13_000_000, transcendentals=0),
        name="merge",
    )(scal, tile, *parts)


def parity_kernel(inten, prop, pick, inten_out, prop_out, mid):
    half = pick.shape[0] // 2

    def sort(src, dst, index):
        x = src[index]
        top = x.astype(jnp.bfloat16)
        rest = x - top.astype(jnp.float32)
        middle = rest.astype(jnp.bfloat16)
        last = (rest - middle.astype(jnp.float32)).astype(jnp.bfloat16)
        out = mm(top, pick[...]) + mm(middle, pick[...]) + mm(last, pick[...])
        mid[2 * index] = out[:, :half]
        mid[2 * index + 1] = out[:, half:]
        for q in range(2):
            for p in range(2):
                cols = slice((2 * q + p) * half, (2 * q + p + 1) * half)
                dst[index, :, cols] = mid[2 * index + p, pl.ds(q, half, stride=2), :]

    for i in range(inten.shape[0]):
        sort(inten, inten_out, i)
    for i in range(prop.shape[0]):
        sort(prop, prop_out, i)


def by_parity(inten, prop):
    frame = inten.shape[-1]
    half = frame // 2
    pick = np.zeros((frame, frame), np.float32)
    n = np.arange(half)
    pick[2 * n, n] = 1.0
    pick[2 * n + 1, half + n] = 1.0
    vmem = pl.BlockSpec(memory_space=pltpu.VMEM)
    return pl.pallas_call(
        parity_kernel,
        out_shape=[
            jax.ShapeDtypeStruct((x.shape[0], half, 2 * frame), jnp.float32) for x in (inten, prop)
        ],
        in_specs=[vmem] * 3,
        out_specs=[vmem] * 2,
        scratch_shapes=[pltpu.VMEM((2 * inten.shape[0], frame, half), jnp.float32)],
        compiler_params=pltpu.CompilerParams(vmem_limit_bytes=12 * 1024 * 1024),
        cost_estimate=pl.CostEstimate(flops=4_000_000_000, bytes_accessed=3_000_000, transcendentals=0),
        name="parity",
    )(inten, prop, pick.astype(jnp.bfloat16))


def pair_route(count, first):
    route = []
    for i in range(first, count - 1, 2):
        route += [(i, i + 1), (i + 1, i)]
    return route


def shards(objects, probe_wave, prop_phase, intensity, offsets, counts):
    frame = intensity.shape[1]
    margin = frame // 2
    size_r, _ = objects.shape[1:]
    nx, ny = lax.axis_size("gx"), lax.axis_size("gy")
    parity = lax.axis_index("gx") % 2
    to_left = [(i, i - 1) for i in range(1, ny)]
    to_right = [(i, i + 1) for i in range(ny - 1)]
    e_route, o_route = pair_route(nx, 0), pair_route(nx, 1)
    e_start = jnp.where(parity == 0, size_r - margin, 0)
    o_start = jnp.where(parity == 0, 0, size_r - margin)

    def band(x, start):
        return lax.dynamic_slice_in_dim(x, start, margin, 1)

    o_band = band(objects, o_start)
    ends = jnp.stack([o_band[:, :, :margin], o_band[:, :, -margin:]])
    oedge = lax.ppermute(ends, "gx", o_route)
    right = lax.ppermute(objects[:, :, :margin], "gy", to_left)
    left = lax.ppermute(objects[:, :, -margin:], "gy", to_right)
    over = lax.ppermute(o_band[:, :, margin:-margin], "gx", o_route)
    first, last = oedge[0], oedge[1]
    rcor = lax.ppermute(first, "gy", to_left)
    lcor = lax.ppermute(last, "gy", to_right)

    waves = jnp.stack([jnp.cos(prop_phase), jnp.sin(prop_phase)])
    inten, waves = by_parity(intensity, waves)
    later, inten = lax.optimization_barrier((objects, inten))
    ext = lax.ppermute(band(later, e_start), "gx", e_route)
    ecor = lax.ppermute(jnp.stack([band(left, e_start), band(right, e_start)]), "gx", e_route)

    scal = jnp.concatenate([counts, parity[None].astype(jnp.int32), offsets.reshape(-1)])
    pieces = [objects, left, right, over, oedge, ext, lcor, rcor, ecor]
    tile, left, right, ledge, redge, over, oedge, ext, ol, orr = run_frames(
        scal, pieces, inten, probe_wave, waves, frame
    )

    ext = lax.ppermute(ext, "gx", e_route)
    ol = lax.ppermute(ol, "gy", to_left)
    orr = lax.ppermute(orr, "gy", to_right)
    left = lax.ppermute(left, "gy", to_left)
    right = lax.ppermute(right, "gy", to_right)
    over = lax.ppermute(over, "gx", o_route)
    ledge = ledge + ext[:, :, :margin]
    redge = redge + ext[:, :, -margin:]
    oedge = oedge + jnp.stack([orr, ol])
    ledge = lax.ppermute(ledge, "gy", to_left)
    redge = lax.ppermute(redge, "gy", to_right)
    oedge = lax.ppermute(oedge, "gx", o_route)
    return merge(scal, tile, left, right, ledge, redge, over, oedge, ext)


def solution(mesh):
    return jax.shard_map(
        shards,
        mesh=mesh,
        in_specs=(
            P(None, "gx", "gy"),
            P(),
            P(),
            P(("gx", "gy"), None, None),
            P(("gx", "gy"), None),
            P(("gx", "gy")),
        ),
        out_specs=P(None, "gx", "gy"),
        check_vma=False,
    )
```

```python
import math

import jax
import jax.numpy as jnp
import numpy as np
from jax import lax
from jax.experimental import pallas as pl
from jax.experimental.pallas import tpu as pltpu
from jax.sharding import PartitionSpec as P


ROWS = 32


def half_tables(frame):
    half = frame // 2
    n = np.arange(half)
    angle = 2.0 * np.pi * ((n[:, None] * n[None, :]) % half) / half
    scale = 1.0 / math.sqrt(frame)
    c, s = np.cos(angle) * scale, np.sin(angle) * scale
    right = np.block([[c, -s], [s, c]])
    turn = 2.0 * np.pi * n / frame
    return right, np.cos(turn), np.sin(turn)


def split_const(m):
    hi = m.astype(np.float32).astype(jnp.bfloat16)
    lo = (m - hi.astype(np.float64)).astype(np.float32).astype(jnp.bfloat16)
    return hi, lo


def mm(left, right):
    return jnp.dot(left, right, preferred_element_type=jnp.float32)


def cmul(ar, ai, br, bi):
    return ar * br - ai * bi, ar * bi + ai * br


def cmul_conj(ar, ai, br, bi):
    return ar * br + ai * bi, ar * bi - ai * br


def frame_kernel(
    side, live_count, spots_in, tile, left, right, over, oedge, ext_e, lcor, rcor, ecor, inten_in, probe_in, prop_in, mats_in, twl_in, twc_in,
    g_tile, g_lmain, g_rmain, g_ledge, g_redge, g_over, g_oedge, g_ext, g_ol, g_or,
    obj, acc, win, car, fld, lh, ll, rh, rl, dd, inten, probe, prop, mats, twl, twc, sems,
):
    frame = probe.shape[1]
    cap = inten.shape[0]
    half = frame // 2
    size = tile.shape[1]
    ntile = size // half
    even = side[0] == 0
    count = live_count[0]
    e_row = jnp.where(even, half + size, 0)
    o_row = jnp.where(even, 0, half + size)
    e_row = pl.multiple_of(e_row, half)
    o_row = pl.multiple_of(o_row, half)
    mid = pl.ds(half, size)

    def blocks(array, width):
        return [array.at[:, :, pl.ds(half * j, half)] for j in range(width)]

    m_row = pl.multiple_of(jnp.where(even, half, frame), half)
    edge_row = pl.multiple_of(jnp.where(even, size, half), half)
    o_rows, e_rows = pl.ds(o_row, half), pl.ds(e_row, half)
    m_rows, edge_rows = pl.ds(m_row, size - half), pl.ds(edge_row, half)
    last = ntile + 1

    def moves(big, t, o, ol, orr, e):
        pairs = [(ol, big.at[:, 0, o_rows, :]), (orr, big.at[:, last, o_rows, :])]
        for j in range(ntile):
            pairs.append((o[j], big.at[:, j + 1, o_rows, :]))
            pairs.append((t[j], big.at[:, j + 1, mid, :]))
        for j in range(ntile + 2):
            pairs.append((e[j], big.at[:, j, e_rows, :]))
        return pairs

    def o_blocks(middle, ends):
        return [ends.at[0]] + blocks(middle, ntile - 2) + [ends.at[1]]

    routes = moves(
        obj, blocks(tile, ntile), o_blocks(over, oedge), lcor, rcor,
        [ecor.at[0]] + blocks(ext_e, ntile) + [ecor.at[1]],
    ) + [
        (left, obj.at[:, 0, mid, :]), (right, obj.at[:, last, mid, :]),
        (inten_in, inten), (probe_in, probe), (prop_in, prop), (mats_in, mats), (twl_in, twl), (twc_in, twc)
    ]
    loads = [pltpu.make_async_copy(src, dst, sems.at[i]) for i, (src, dst) in enumerate(routes)]
    for copy in loads:
        copy.start()

    def clear(i, carry):
        acc[i // (ntile + 2), i % (ntile + 2)] = jnp.zeros(acc.shape[2:], jnp.float32)
        return carry

    lax.fori_loop(0, acc.shape[0] * (ntile + 2), clear, 0)
    for copy in loads:
        copy.wait()

    lane = lax.broadcasted_iota(jnp.int32, (ROWS, half), 1)
    low, high = slice(0, half), slice(half, frame)

    def put(hi_ref, lo_ref, u, rows, cols, value):
        hi = value.astype(jnp.bfloat16)
        hi_ref[u, rows, cols] = hi
        lo_ref[u, rows, cols] = (value - hi.astype(jnp.float32)).astype(jnp.bfloat16)

    def right_product(u, m):
        dd[u] = mm(lh[u], mats[m]) + mm(ll[u], mats[m]) + mm(lh[u], mats[m + 1])

    def left_product(u, m):
        fld[u] = mm(mats[m], rh[u]) + mm(mats[m], rl[u]) + mm(mats[m + 1], rh[u])

    def right_forward(u, source):
        for rb in range(0, frame, ROWS):
            rows = slice(rb, rb + ROWS)
            xr, xi = source(u, rows)
            ar, br, ai, bi = xr[:, :half], xr[:, half:], xi[:, :half], xi[:, half:]
            put(lh, ll, u, rows, low, ar + br)
            put(lh, ll, u, rows, high, ai + bi)
            dr, di = ar - br, ai - bi
            c, s = twl[0:1, :], twl[1:2, :]
            vrows = slice(frame + rb, frame + rb + ROWS)
            put(lh, ll, u, vrows, low, dr * c + di * s)
            put(lh, ll, u, vrows, high, di * c - dr * s)
        right_product(u, 0)

    def left_forward(u):
        for q in range(2):
            for rb in range(0, half, ROWS):
                rows = slice(rb, rb + ROWS)
                t = slice(q * frame + rb, q * frame + rb + ROWS)
                b = slice(q * frame + half + rb, q * frame + half + rb + ROWS)
                ar, ai, br, bi = dd[u, t, low], dd[u, t, high], dd[u, b, low], dd[u, b, high]
                irows = slice(half + rb, half + rb + ROWS)
                ucols = slice(q * half, (q + 1) * half)
                vcols = slice(frame + q * half, frame + (q + 1) * half)
                put(rh, rl, u, rows, ucols, ar + br)
                put(rh, rl, u, irows, ucols, ai + bi)
                dr, di = ar - br, ai - bi
                c, s = twc[0, rows, :], twc[1, rows, :]
                put(rh, rl, u, rows, vcols, dr * c + di * s)
                put(rh, rl, u, irows, vcols, di * c - dr * s)
        left_product(u, 2)

    def left_inverse(u, source):
        for rb in range(0, half, ROWS):
            rows = slice(rb, rb + ROWS)
            xr, xi = source(u, rows)
            put(rh, rl, u, rows, slice(None), xr)
            put(rh, rl, u, slice(half + rb, half + rb + ROWS), slice(None), xi)
        left_product(u, 0)

    def right_inverse(u):
        for q in range(2):
            for rb in range(0, half, ROWS):
                rows = slice(rb, rb + ROWS)
                irows = slice(half + rb, half + rb + ROWS)
                ecols = slice(q * half, (q + 1) * half)
                ocols = slice(frame + q * half, frame + (q + 1) * half)
                er, ei = fld[u, rows, ecols], fld[u, irows, ecols]
                wr, wi = fld[u, rows, ocols], fld[u, irows, ocols]
                c, s = twc[0, rows, :], twc[1, rows, :]
                tr, ti = wr * c - wi * s, wi * c + wr * s
                top = slice(q * frame + rb, q * frame + rb + ROWS)
                bot = slice(q * frame + half + rb, q * frame + half + rb + ROWS)
                put(lh, ll, u, top, low, er + tr)
                put(lh, ll, u, top, high, ei + ti)
                put(lh, ll, u, bot, low, er - tr)
                put(lh, ll, u, bot, high, ei - ti)
        right_product(u, 2)

    def finish(u, sink):
        for rb in range(0, frame, ROWS):
            rows = slice(rb, rb + ROWS)
            orows = slice(frame + rb, frame + rb + ROWS)
            er, ei, wr, wi = dd[u, rows, low], dd[u, rows, high], dd[u, orows, low], dd[u, orows, high]
            c, s = twl[0:1, :], twl[1:2, :]
            tr, ti = wr * c - wi * s, wi * c + wr * s
            sink(u, rows, er + tr, ei + ti, er - tr, ei - ti)

    def step(i, carry):
        first = 2 * i
        slots = (first, jnp.minimum(first + 1, cap - 1))
        live = (None, first + 1 < count)
        spots = []
        for slot in slots:
            r, c = spots_in[0, slot], spots_in[1, slot]
            j = jnp.minimum(c // half, ntile - 1)
            cs = c - j * half
            spots.append((r, j, cs, lax.rem(half - cs, half), lax.rem(cs, half)))

        def load(u, k):
            r, j, cs, back, _ = spots[u]
            keep = lane + cs < half
            for rb in range(0, frame, ROWS):
                parts = [
                    pltpu.roll(obj[k, j + t, pl.ds(r + rb, ROWS), :], back, 1) for t in range(3)
                ]
                win[u, k, rb:rb + ROWS, low] = jnp.where(keep, parts[0], parts[1])
                win[u, k, rb:rb + ROWS, high] = jnp.where(keep, parts[1], parts[2])

        def place(u, k, rows, first, second):
            r, j, cs, _, fore = spots[u]
            zero = jnp.zeros_like(first)
            if live[u] is not None:
                first = jnp.where(live[u], first, zero)
                second = jnp.where(live[u], second, zero)
            spill = lane >= cs
            a, b = pltpu.roll(first, fore, 1), pltpu.roll(second, fore, 1)
            at = pl.ds(r + rows.start, ROWS)
            acc[k, j, at, :] += jnp.where(spill, a, zero)
            acc[k, j + 1, at, :] += jnp.where(spill, b, a)
            acc[k, j + 2, at, :] += jnp.where(spill, zero, b)

        def lower(rows):
            return slice(half + rows.start, half + rows.stop)

        def enter(u, rows):
            return cmul(probe[0, rows, :], probe[1, rows, :], win[u, 0, rows, :], win[u, 1, rows, :])

        def propagate(u, rows):
            return cmul(prop[0, rows, :], prop[1, rows, :], fld[u, rows, :], fld[u, lower(rows), :])

        def propagate_back(u, rows):
            return cmul_conj(prop[0, rows, :], prop[1, rows, :], fld[u, rows, :], fld[u, lower(rows), :])

        def carried(u, rows, ar, ai, br, bi):
            car[u, 0, rows, low] = ar
            car[u, 1, rows, low] = ai
            car[u, 0, rows, high] = br
            car[u, 1, rows, high] = bi

        def exit_wave(u, rows):
            return cmul(car[u, 0, rows, :], car[u, 1, rows, :], win[u, 2, rows, :], win[u, 3, rows, :])

        def misfit(u, rows):
            fr, fi = fld[u, rows, :], fld[u, lower(rows), :]
            m = fr * fr + fi * fi - inten[slots[u], rows, :]
            return m * fr, m * fi

        def grad_exit(u, rows, ar, ai, br, bi):
            lr, li = cmul_conj(car[u, 0, rows, low], car[u, 1, rows, low], ar, ai)
            hr, hi = cmul_conj(car[u, 0, rows, high], car[u, 1, rows, high], br, bi)
            place(u, 2, rows, lr, hr)
            place(u, 3, rows, li, hi)
            for cols, (gr, gi) in ((low, (ar, ai)), (high, (br, bi))):
                xr, xi = cmul_conj(win[u, 2, rows, cols], win[u, 3, rows, cols], gr, gi)
                win[u, 0, rows, cols] = xr
                win[u, 1, rows, cols] = xi

        def inner(u, rows):
            return win[u, 0, rows, :], win[u, 1, rows, :]

        def grad_enter(u, rows, ar, ai, br, bi):
            lr, li = cmul_conj(probe[0, rows, low], probe[1, rows, low], ar, ai)
            hr, hi = cmul_conj(probe[0, rows, high], probe[1, rows, high], br, bi)
            place(u, 0, rows, lr, hr)
            place(u, 1, rows, li, hi)

        both = (0, 1)
        phases = [
            lambda u: [load(u, 0), load(u, 1), right_forward(u, enter)],
            left_forward,
            lambda u: left_inverse(u, propagate),
            right_inverse,
            lambda u: [finish(u, carried), load(u, 2), load(u, 3), right_forward(u, exit_wave)],
            left_forward,
            lambda u: left_inverse(u, misfit),
            right_inverse,
            lambda u: [finish(u, grad_exit), right_forward(u, inner)],
            left_forward,
            lambda u: left_inverse(u, propagate_back),
            right_inverse,
            lambda u: finish(u, grad_enter),
        ]
        for phase in phases:
            for u in both:
                phase(u)
        return carry

    lax.fori_loop(0, (count + 1) // 2, step, 0)

    targets = moves(
        acc, blocks(g_tile, ntile), o_blocks(g_over, g_oedge), g_ol, g_or, blocks(g_ext, ntile + 2)
    ) + [
        (g_lmain, acc.at[:, 0, m_rows, :]), (g_rmain, acc.at[:, last, m_rows, :]),
        (g_ledge, acc.at[:, 0, edge_rows, :]), (g_redge, acc.at[:, last, edge_rows, :]),
    ]
    stores = [pltpu.make_async_copy(src, dst, sems.at[i]) for i, (dst, src) in enumerate(targets)]
    for copy in stores:
        copy.start()
    for copy in stores:
        copy.wait()


def run_frames(scalars, pieces, inten, probe, prop, frame):
    right, tc, ts = half_tables(frame)
    half = frame // 2
    rhi, rlo = split_const(right)
    mats = np.stack([rhi, rlo, np.ascontiguousarray(rhi.T), np.ascontiguousarray(rlo.T)])
    twl = np.zeros((8, half), np.float32)
    twl[0], twl[1] = tc, ts
    twc = np.stack([np.repeat(tc[:, None], half, 1), np.repeat(ts[:, None], half, 1)]).astype(np.float32)
    channels, size, _ = pieces[0].shape
    ntile = size // half
    hbm = pl.BlockSpec(memory_space=pl.ANY)
    vmem = pl.BlockSpec(memory_space=pltpu.VMEM)
    big = (channels, ntile + 2, size + frame, half)
    tile, _, _, over, oedge, _, cor = pieces[:7]
    main = (channels, size - half, half)
    strip = (channels, half, size + frame)
    outs = [
        jax.ShapeDtypeStruct(shape, jnp.float32)
        for shape in (
            tile.shape, main, main, cor.shape, cor.shape, over.shape, oedge.shape, strip, cor.shape, cor.shape
        )
    ]
    operands = (inten, probe, prop, mats, twl, twc)
    copies = 3 * ntile + 8 + len(operands)
    return pl.pallas_call(
        frame_kernel,
        out_shape=outs,
        in_specs=[pl.BlockSpec(memory_space=pltpu.SMEM)] * len(scalars) + [hbm] * len(pieces) + [pl.BlockSpec(memory_space=pltpu.HBM)] * len(operands),
        out_specs=[hbm] * len(outs),
        scratch_shapes=[
            pltpu.VMEM(big, jnp.float32),
            pltpu.VMEM(big, jnp.float32),
            pltpu.VMEM((2, 4, frame, frame), jnp.float32),
            pltpu.VMEM((2, 2, frame, frame), jnp.float32),
            pltpu.VMEM((2, frame, 2 * frame), jnp.float32),
            pltpu.VMEM((2, 2 * frame, frame), jnp.bfloat16),
            pltpu.VMEM((2, 2 * frame, frame), jnp.bfloat16),
            pltpu.VMEM((2, frame, 2 * frame), jnp.bfloat16),
            pltpu.VMEM((2, frame, 2 * frame), jnp.bfloat16),
            pltpu.VMEM((2, 2 * frame, frame), jnp.float32),
        ]
        + [pltpu.VMEM(x.shape, x.dtype) for x in operands]
        + [pltpu.SemaphoreType.DMA((copies,))],
        compiler_params=pltpu.CompilerParams(vmem_limit_bytes=31 * 1024 * 1024),
        cost_estimate=pl.CostEstimate(flops=40_000_000_000, bytes_accessed=30_000_000, transcendentals=0),
        name="frames",
    )(*scalars, *pieces, *operands)


def merge_kernel(side, tile, right, left, redge, ledge, over, oedge, ext, out, stage, sems):
    channels, size, _ = stage.shape
    w = right.shape[2]
    even = side[0] == 0
    far = size - w
    e_row = pl.multiple_of(jnp.where(even, far, 0), w)
    o_row = pl.multiple_of(jnp.where(even, 0, far), w)
    m_row = pl.multiple_of(jnp.where(even, 0, w), w)
    lo, mid, hi = slice(0, w), slice(w, far), slice(far, size)
    e_rows, o_rows, m_rows = pl.ds(e_row, w), pl.ds(o_row, w), pl.ds(m_row, far)
    copies = []
    for k in range(channels):
        stage[k] = tile[k]
        stage[k, m_rows, hi] += right[k]
        stage[k, m_rows, lo] += left[k]
        stage[k, o_rows, mid] += over[k]
        stage[k, o_rows, lo] += oedge[0, k]
        stage[k, o_rows, hi] += oedge[1, k]
        stage[k, e_rows, :] += ext[k, :, w:-w]
        stage[k, e_rows, hi] += redge[k]
        stage[k, e_rows, lo] += ledge[k]
        copy = pltpu.make_async_copy(stage.at[k], out.at[k], sems.at[k])
        copy.start()
        copies.append(copy)
    for copy in copies:
        copy.wait()


def merge(side, tile, *parts):
    vmem = pl.BlockSpec(memory_space=pltpu.VMEM)
    return pl.pallas_call(
        merge_kernel,
        out_shape=jax.ShapeDtypeStruct(tile.shape, jnp.float32),
        in_specs=[pl.BlockSpec(memory_space=pltpu.SMEM)] + [vmem] * (1 + len(parts)),
        out_specs=pl.BlockSpec(memory_space=pl.ANY),
        scratch_shapes=[
            pltpu.VMEM(tile.shape, jnp.float32),
            pltpu.SemaphoreType.DMA((tile.shape[0],)),
        ],
        compiler_params=pltpu.CompilerParams(vmem_limit_bytes=20 * 1024 * 1024),
        cost_estimate=pl.CostEstimate(flops=10_000_000, bytes_accessed=13_000_000, transcendentals=0),
        name="merge",
    )(side, tile, *parts)


def parity_kernel(inten, prop, pick, inten_out, prop_out, mid):
    half = pick.shape[0] // 2

    def sort(src, dst, index):
        x = src[index]
        top = x.astype(jnp.bfloat16)
        rest = x - top.astype(jnp.float32)
        middle = rest.astype(jnp.bfloat16)
        last = (rest - middle.astype(jnp.float32)).astype(jnp.bfloat16)
        out = mm(top, pick[...]) + mm(middle, pick[...]) + mm(last, pick[...])
        mid[2 * index] = out[:, :half]
        mid[2 * index + 1] = out[:, half:]
        for q in range(2):
            for p in range(2):
                cols = slice((2 * q + p) * half, (2 * q + p + 1) * half)
                dst[index, :, cols] = mid[2 * index + p, pl.ds(q, half, stride=2), :]

    for i in range(inten.shape[0]):
        sort(inten, inten_out, i)
    for i in range(prop.shape[0]):
        sort(prop, prop_out, i)


def by_parity(inten, prop):
    frame = inten.shape[-1]
    half = frame // 2
    pick = np.zeros((frame, frame), np.float32)
    n = np.arange(half)
    pick[2 * n, n] = 1.0
    pick[2 * n + 1, half + n] = 1.0
    vmem = pl.BlockSpec(memory_space=pltpu.VMEM)
    return pl.pallas_call(
        parity_kernel,
        out_shape=[
            jax.ShapeDtypeStruct((x.shape[0], half, 2 * frame), jnp.float32) for x in (inten, prop)
        ],
        in_specs=[vmem] * 3,
        out_specs=[vmem] * 2,
        scratch_shapes=[pltpu.VMEM((2 * inten.shape[0], frame, half), jnp.float32)],
        compiler_params=pltpu.CompilerParams(vmem_limit_bytes=6 * 1024 * 1024),
        cost_estimate=pl.CostEstimate(flops=4_000_000_000, bytes_accessed=3_000_000, transcendentals=0),
        name="parity",
    )(inten, prop, pick.astype(jnp.bfloat16))


def cut_kernel(side, tile, first, last, o_mid, o_ends, e_band, sems):
    size = tile.shape[1]
    w = first.shape[2]
    far = size - w
    even = side[0] == 0
    e_rows = pl.ds(pl.multiple_of(jnp.where(even, far, 0), w), w)
    o_rows = pl.ds(pl.multiple_of(jnp.where(even, 0, far), w), w)
    lo, mid, hi = pl.ds(0, w), pl.ds(w, far - w), pl.ds(far, w)
    routes = [
        (tile.at[:, :, lo], first),
        (tile.at[:, :, hi], last),
        (tile.at[:, o_rows, lo], o_ends.at[0]),
        (tile.at[:, o_rows, hi], o_ends.at[1]),
        (tile.at[:, o_rows, mid], o_mid),
        (tile.at[:, e_rows, :], e_band),
    ]
    copies = [pltpu.make_async_copy(src, dst, sems.at[i]) for i, (src, dst) in enumerate(routes)]
    for copy in copies:
        copy.start()
    for copy in copies:
        copy.wait()


def cut(side, tile, w):
    channels, size, _ = tile.shape
    shapes = (
        (channels, size, w), (channels, size, w), (channels, w, size - 2 * w),
        (2, channels, w, w), (channels, w, size),
    )
    return pl.pallas_call(
        cut_kernel,
        out_shape=[jax.ShapeDtypeStruct(shape, jnp.float32) for shape in shapes],
        in_specs=[pl.BlockSpec(memory_space=pltpu.SMEM), pl.BlockSpec(memory_space=pl.ANY)],
        out_specs=[pl.BlockSpec(memory_space=pltpu.VMEM)] * len(shapes),
        scratch_shapes=[pltpu.SemaphoreType.DMA((6,))],
        compiler_params=pltpu.CompilerParams(vmem_limit_bytes=8 * 1024 * 1024),
        cost_estimate=pl.CostEstimate(flops=1_000_000, bytes_accessed=8_000_000, transcendentals=0),
        name="cut",
    )(side, tile)


def ends_kernel(side, left, right, out):
    w = out.shape[2]
    rows = pl.ds(pl.multiple_of(jnp.where(side[0] == 0, left.shape[1] - w, 0), w), w)
    for k in range(out.shape[1]):
        out[0, k] = left[k, rows, :]
        out[1, k] = right[k, rows, :]


def edge_ends(side, left, right):
    channels, _, w = left.shape
    vmem = pl.BlockSpec(memory_space=pltpu.VMEM)
    return pl.pallas_call(
        ends_kernel,
        out_shape=jax.ShapeDtypeStruct((2, channels, w, w), jnp.float32),
        in_specs=[pl.BlockSpec(memory_space=pltpu.SMEM), vmem, vmem],
        out_specs=vmem,
        compiler_params=pltpu.CompilerParams(vmem_limit_bytes=8 * 1024 * 1024),
        cost_estimate=pl.CostEstimate(flops=1_000_000, bytes_accessed=1_000_000, transcendentals=0),
        name="ends",
    )(side, left, right)


def pair_route(count, first):
    route = []
    for i in range(first, count - 1, 2):
        route += [(i, i + 1), (i + 1, i)]
    return route


def shards(objects, probe_wave, prop_phase, intensity, offsets, counts):
    frame = intensity.shape[1]
    margin = frame // 2
    nx, ny = lax.axis_size("gx"), lax.axis_size("gy")
    parity = lax.axis_index("gx") % 2
    to_left = [(i, i - 1) for i in range(1, ny)]
    to_right = [(i, i + 1) for i in range(ny - 1)]
    e_route, o_route = pair_route(nx, 0), pair_route(nx, 1)

    side = parity[None].astype(jnp.int32)
    first, last, o_mid, o_ends, e_band = cut(side, objects, margin)
    right = lax.ppermute(first, "gy", to_left)
    left = lax.ppermute(last, "gy", to_right)
    oedge = lax.ppermute(o_ends, "gx", o_route)
    over = lax.ppermute(o_mid, "gx", o_route)
    ext = lax.ppermute(e_band, "gx", e_route)
    first, last = oedge[0], oedge[1]
    rcor = lax.ppermute(first, "gy", to_left)
    lcor = lax.ppermute(last, "gy", to_right)

    waves = jnp.stack([jnp.cos(prop_phase), jnp.sin(prop_phase)])
    inten, waves = by_parity(intensity, waves)
    ends = edge_ends(side, left, right)
    ecor = lax.ppermute(ends, "gx", e_route)

    pieces = [objects, left, right, over, oedge, ext, lcor, rcor, ecor]
    tile, left, right, ledge, redge, over, oedge, ext, ol, orr = run_frames(
        (side, counts, offsets.T), pieces, inten, probe_wave, waves, frame
    )

    ext = lax.ppermute(ext, "gx", e_route)
    ol = lax.ppermute(ol, "gy", to_left)
    orr = lax.ppermute(orr, "gy", to_right)
    left = lax.ppermute(left, "gy", to_left)
    right = lax.ppermute(right, "gy", to_right)
    over = lax.ppermute(over, "gx", o_route)
    ledge = ledge + ext[:, :, :margin]
    redge = redge + ext[:, :, -margin:]
    oedge = oedge + jnp.stack([orr, ol])
    ledge = lax.ppermute(ledge, "gy", to_left)
    redge = lax.ppermute(redge, "gy", to_right)
    oedge = lax.ppermute(oedge, "gx", o_route)
    return merge(side, tile, left, right, ledge, redge, over, oedge, ext)


def solution(mesh):
    return jax.shard_map(
        shards,
        mesh=mesh,
        in_specs=(
            P(None, "gx", "gy"),
            P(),
            P(),
            P(("gx", "gy"), None, None),
            P(("gx", "gy"), None),
            P(("gx", "gy")),
        ),
        out_specs=P(None, "gx", "gy"),
        check_vma=False,
    )
```
